32 devices in a mesh: dp: 4 (over x, y), sp: 8 (over z, core).
Axes of the slice: x: 2, y: 2, z: 4, core: 2. Of those that a mesh axis runs over, the one named last changes fastest.
Arguments:
- q: bfloat16 [128, 16, 128], P('dp'), parts along dimension 0
- k: bfloat16 [128, 4096, 16, 128], P('dp', 'sp'), parts along dimension 0
- v: bfloat16 [128, 4096, 16, 128], P('dp', 'sp'), parts along dimension 0
Outputs:
- q: bfloat16 [128, 16, 128], P('dp'), parts along dimension 0
There are 4 independent parts. The reference program is written for one: setup_inputs(seed, part) draws one part's arguments, and reference() takes and returns one part's arrays. A program takes and returns all parts, laid end to end along the dimension named above; each array names one.
All inputs are finite; a program needn't handle non-finite values.
Results may differ from the reference program's by a relative error of at most 0.012.
Values are sent between devices in bfloat16 or wider.
A program may use at most 2 GiB of HBM per device.

```python
import jax
import jax.numpy as jnp

BATCH = 32
CACHE = 4096
HEADS = 16
KV_HEADS = 16
HEAD = 128


def setup_inputs(seed: int = 0, part: int = 0) -> dict:
    kq, kk, kv = (jax.random.fold_in(k, part) for k in jax.random.split(jax.random.key(seed), 3))
    return {
        "q": (3 * jax.random.normal(kq, (BATCH, HEADS, HEAD), jnp.float32)).astype(jnp.bfloat16),
        "k": jax.random.normal(kk, (BATCH, CACHE, KV_HEADS, HEAD), jnp.float32).astype(jnp.bfloat16),
        "v": jax.random.normal(kv, (BATCH, CACHE, KV_HEADS, HEAD), jnp.float32).astype(jnp.bfloat16),
    }


def einsum(form, a, b):
    return jnp.einsum(form, a.astype(jnp.float32), b.astype(jnp.float32))


def reference(q, k, v):
    grouped = q.reshape(BATCH, KV_HEADS, -1, HEAD)
    scores = einsum("bgsd,bugd->bgsu", grouped, k) * HEAD**-0.5
    weights = jax.nn.softmax(scores, -1).astype(jnp.bfloat16)
    return einsum("bgsu,bugd->bgsd", weights, v).astype(jnp.bfloat16).reshape(BATCH, HEADS, HEAD)
```

```python
import functools

import jax
import jax.numpy as jnp
from jax import lax
from jax.experimental import pallas as pl
from jax.experimental.pallas import tpu as pltpu
from jax.sharding import PartitionSpec as P

SLOTS = 6
TILE = 8
PER = 4


def attend(n, q_ref, k_hbm, v_hbm, o_ref, k_buf, v_buf, s_ref, p_ref, part, stat, last_part, last_stat, k_sem, v_sem,
           send_sem, part_sem, stat_sem, last_send_sem, last_part_sem, last_stat_sem):
    batch, tokens, heads, head = k_hbm.shape
    runs = tokens // TILE
    groups = batch // PER - 1
    me = lax.axis_index("sp")
    scale = head**-0.5
    lanes = lax.broadcasted_iota(jnp.int32, (heads, TILE * heads), 1)
    mine = lanes % heads == lax.broadcasted_iota(jnp.int32, (heads, TILE * heads), 0)
    lane = lax.broadcasted_iota(jnp.int32, (8, 128), 1)

    def k_copy(b):
        slot = lax.rem(b, SLOTS)
        return pltpu.make_async_copy(k_hbm.at[b], k_buf.at[slot], k_sem.at[slot])

    def v_copy(b):
        slot = lax.rem(b, SLOTS)
        return pltpu.make_async_copy(v_hbm.at[b], v_buf.at[slot], v_sem.at[slot])

    def scores(b):
        keys = k_buf.at[lax.rem(b, SLOTS)].reshape(runs, TILE, heads, head)
        query = q_ref[b]
        none = jnp.zeros_like(query)
        high = jnp.full((heads, TILE * heads), -jnp.inf, jnp.float32)
        step = 16
        for m in range(0, runs, step):
            total = None
            for j in range(0, TILE, 2):
                pair = jnp.concatenate([keys[m : m + step, j + c].reshape(step * heads, head) for c in range(2)], 1)
                spread = jnp.concatenate(
                    [jnp.concatenate([query if r == j + c else none for c in range(2)], 1) for r in range(TILE)], 0
                )
                term = lax.dot_general(pair, spread, (((1,), (1,)), ((), ())), preferred_element_type=jnp.float32)
                total = term if total is None else total + term
            total = jnp.where(mine[None], total.reshape(step, heads, TILE * heads), -jnp.inf)
            s_ref[m : m + step] = total
            high = jnp.maximum(high, jnp.max(total, 0))
        return jnp.max(high, 1, keepdims=True) * scale

    def weights(high):
        total = jnp.zeros((heads, TILE * heads), jnp.float32)
        for m in range(runs):
            weight = jnp.exp(s_ref[m] * scale - high)
            total = total + weight
            p_ref[m] = weight.astype(jnp.bfloat16)
        return jnp.sum(total, 1, keepdims=True)

    def values(b):
        rows = v_buf.at[lax.rem(b, SLOTS)].reshape(tokens * heads, head)
        half, deep = tokens * heads // 2, 2 * TILE * heads
        total = None
        for t in range(runs // 4):
            weight = jnp.concatenate(
                [jnp.concatenate([p_ref[x + 2 * t], p_ref[x + 2 * t + 1]], 1) for x in (0, runs // 2)], 0
            )
            value = jnp.concatenate([rows[x + deep * t : x + deep * (t + 1)] for x in (0, half)], 1)
            term = jnp.dot(weight, value, preferred_element_type=jnp.float32)
            total = term if total is None else total + term
        return total[:heads, :head] + total[heads:, head:]

    def noted(table, i, high, total):
        for part_of_heads in range(2):
            rows = slice(8 * part_of_heads, 8 * part_of_heads + 8)
            table = jnp.where(lane == 2 * i + part_of_heads, high[rows], table)
            table = jnp.where(lane == 64 + 2 * i + part_of_heads, total[rows], table)
        return table

    def sends(parts, stats, g, send, part_recv, stat_recv):
        copies = []
        for r in range(1, n):
            peer = {"sp": lax.rem(me + r, n)}
            for buf, recv, s in ((parts, part_recv, 0), (stats, stat_recv, 1)):
                copies.append(
                    pltpu.make_async_remote_copy(
                        src_ref=buf.at[g, me],
                        dst_ref=buf.at[g, me],
                        send_sem=send.at[s],
                        recv_sem=recv.at[g],
                        device_id=peer,
                        device_id_type=pl.DeviceIdType.MESH,
                    )
                )
        return copies

    def arrived(parts, stats, g, part_recv, stat_recv):
        pltpu.make_async_copy(parts.at[g, : n - 1], parts.at[g, : n - 1], part_recv.at[g]).wait()
        pltpu.make_async_copy(stats.at[g, : n - 1], stats.at[g, : n - 1], stat_recv.at[g]).wait()

    def together(parts, stats, g, first, count):
        tables = [stats[g, d] for d in range(n)]
        high = functools.reduce(jnp.maximum, tables)
        shares = [jnp.exp(t - high) for t in tables]
        total = functools.reduce(jnp.add, [pltpu.roll(t, 64, 1) * s for t, s in zip(tables, shares)])
        for i in range(count):
            out = []
            for x in range(2):
                column = 2 * i + x
                seen = None
                for d in range(n):
                    rows = slice(i * heads + 8 * x, i * heads + 8 * x + 8)
                    term = parts[g, d, i * heads : (i + 1) * heads].astype(jnp.float32)[8 * x : 8 * x + 8] * shares[d][:, column : column + 1]
                    seen = term if seen is None else seen + term
                out.append(seen / total[:, column : column + 1])
            o_ref[first + i] = jnp.concatenate(out, 0).astype(jnp.bfloat16)

    barrier = pltpu.get_barrier_semaphore()
    for r in range(1, n):
        pl.semaphore_signal(barrier, inc=1, device_id={"sp": lax.rem(me + r, n)}, device_id_type=pl.DeviceIdType.MESH)
    for b in range(SLOTS):
        k_copy(b).start()
        if b:
            v_copy(b - 1).start()

    def more(b):
        @pl.when(b + SLOTS < batch)
        def _():
            k_copy(b + SLOTS).start()

        @pl.when(b + SLOTS - 1 < batch)
        def _():
            v_copy(b + SLOTS - 1).start()

    k_copy(0).wait()
    high = scores(0)
    total = weights(high)
    more(0)
    pl.semaphore_wait(barrier, n - 1)

    def sequence(b, high, total):
        k_copy(b + 1).wait()
        v_copy(b).wait()
        next_high = scores(b + 1)
        seen = values(b)
        next_total = weights(next_high)
        more(b + 1)
        return seen, next_high, next_total

    def group(g, carry):
        high, total = carry
        table = jnp.zeros((8, 128), jnp.float32)
        for i in range(PER):
            table = noted(table, i, high, total)
            seen, high, total = sequence(g * PER + i, high, total)
            part[g, me, i * heads : (i + 1) * heads] = seen.astype(jnp.bfloat16)
        stat[g, me] = table
        for copy in sends(part, stat, g, send_sem, part_sem, stat_sem):
            copy.start()

        @pl.when(g > 0)
        def _():
            arrived(part, stat, g - 1, part_sem, stat_sem)
            together(part, stat, g - 1, (g - 1) * PER, PER)

        return high, total

    high, total = lax.fori_loop(0, groups, group, (high, total))
    for i in range(PER):
        b = groups * PER + i
        last_stat[i, me] = noted(jnp.zeros((8, 128), jnp.float32), 0, high, total)
        if i < PER - 1:
            seen, high, total = sequence(b, high, total)
        else:
            v_copy(b).wait()
            seen = values(b)
        last_part[i, me] = seen.astype(jnp.bfloat16)
        for copy in sends(last_part, last_stat, i, last_send_sem, last_part_sem, last_stat_sem):
            copy.start()
    arrived(part, stat, groups - 1, part_sem, stat_sem)
    together(part, stat, groups - 1, (groups - 1) * PER, PER)
    for i in range(PER):
        arrived(last_part, last_stat, i, last_part_sem, last_stat_sem)
        together(last_part, last_stat, i, groups * PER + i, 1)
    for parts, stats, send in ((part, stat, send_sem), (last_part, last_stat, last_send_sem)):
        for s, buf in enumerate((parts, stats)):
            pltpu.make_async_copy(buf.at[:, : n - 1], buf.at[:, : n - 1], send.at[s]).wait()


def solution(mesh):
    n = mesh.shape["sp"]

    def step(q, k, v):
        batch, tokens, heads, head = k.shape
        groups = batch // PER - 1
        anywhere, vmem = pl.BlockSpec(memory_space=pl.ANY), pl.BlockSpec(memory_space=pltpu.VMEM)
        return pl.pallas_call(
            functools.partial(attend, n),
            out_shape=jax.ShapeDtypeStruct(q.shape, q.dtype),
            in_specs=[vmem, anywhere, anywhere],
            out_specs=vmem,
            scratch_shapes=[
                pltpu.VMEM((SLOTS, tokens, heads, head), jnp.bfloat16),
                pltpu.VMEM((SLOTS, tokens, heads, head), jnp.bfloat16),
                pltpu.VMEM((tokens // TILE, heads, TILE * heads), jnp.float32),
                pltpu.VMEM((tokens // TILE, heads, TILE * heads), jnp.bfloat16),
                pltpu.VMEM((groups, n, PER * heads, head), jnp.bfloat16),
                pltpu.VMEM((groups, n, 8, 128), jnp.float32),
                pltpu.VMEM((PER, n, heads, head), jnp.bfloat16),
                pltpu.VMEM((PER, n, 8, 128), jnp.float32),
                pltpu.SemaphoreType.DMA((SLOTS,)),
                pltpu.SemaphoreType.DMA((SLOTS,)),
                pltpu.SemaphoreType.DMA((2,)),
                pltpu.SemaphoreType.DMA((groups,)),
                pltpu.SemaphoreType.DMA((groups,)),
                pltpu.SemaphoreType.DMA((2,)),
                pltpu.SemaphoreType.DMA((PER,)),
                pltpu.SemaphoreType.DMA((PER,)),
            ],
            compiler_params=pltpu.CompilerParams(
                vmem_limit_bytes=60 << 20, collective_id=0, has_side_effects=True
            ),
            name="attend",
        )(q, k, v)

    return jax.shard_map(
        step,
        mesh=mesh,
        in_specs=(P("dp", None, None), P("dp", "sp", None, None), P("dp", "sp", None, None)),
        out_specs=P("dp", None, None),
        check_vma=False,
    )
```

```python
import functools
import math

import jax
import jax.numpy as jnp
from jax import lax
from jax.experimental import pallas as pl
from jax.experimental.pallas import tpu as pltpu
from jax.sharding import PartitionSpec as P

TILE = 8
STEP = 32
PAIR = 2
LAG = 6
SLOTS = 8


def attend(n, q_hbm, k_hbm, v_hbm, o_ref, q_ref, k_buf, v_buf, s_buf, p_buf, part, last, stat, q_sem, k_sem, v_sem,
           send_sem, part_sem, last_sem, stat_sem):
    batch, tokens, heads, head = k_hbm.shape
    runs = tokens // TILE
    pairs = batch // PAIR - 1
    half = batch // 2
    me = lax.axis_index("sp")
    scale = head**-0.5 / math.log(2)
    lanes = lax.broadcasted_iota(jnp.int32, (heads, TILE * heads), 1)
    mine = lanes % heads == lax.broadcasted_iota(jnp.int32, (heads, TILE * heads), 0)
    lane = lax.broadcasted_iota(jnp.int32, (8, 128), 1)

    def k_copy(b):
        slot = lax.rem(b, SLOTS)
        return pltpu.make_async_copy(k_hbm.at[b], k_buf.at[slot], k_sem.at[slot])

    def v_copy(b):
        slot = lax.rem(b, SLOTS)
        return pltpu.make_async_copy(v_hbm.at[b], v_buf.at[slot], v_sem.at[slot])

    def scores(b, s_ref):
        keys = k_buf.at[lax.rem(b, SLOTS)].reshape(runs, TILE, heads, head)
        query = q_ref[b]
        none = jnp.zeros_like(query)
        high = jnp.full((heads, TILE * heads), -jnp.inf, jnp.float32)
        for m in range(0, runs, STEP):
            total = None
            for j in range(0, TILE, 2):
                two = jnp.concatenate([keys[m : m + STEP, j + c].reshape(STEP * heads, head) for c in range(2)], 1)
                spread = jnp.concatenate(
                    [jnp.concatenate([query if r == j + c else none for c in range(2)], 1) for r in range(TILE)], 0
                )
                term = lax.dot_general(two, spread, (((1,), (1,)), ((), ())), preferred_element_type=jnp.float32)
                total = term if total is None else total + term
            total = jnp.where(mine[None], total.reshape(STEP, heads, TILE * heads), -jnp.inf)
            s_ref[m : m + STEP] = total
            high = jnp.maximum(high, jnp.max(total, 0))
        return jnp.max(high, 1, keepdims=True) * scale

    def weights(high, s_ref, p_ref):
        total = jnp.zeros((heads, TILE * heads), jnp.float32)
        high = jnp.broadcast_to(high, total.shape)
        for m in range(runs):
            weight = jnp.exp2(s_ref[m] * scale - high)
            total = total + weight
            p_ref[m] = weight.astype(jnp.bfloat16)
        return jnp.sum(total, 1, keepdims=True)

    def values(b, p_ref):
        rows = v_buf.at[lax.rem(b, SLOTS)].reshape(tokens * heads, head)
        deep = 2 * TILE * heads
        total = None
        for t in range(0, runs, 4):
            weight = jnp.concatenate([jnp.concatenate([p_ref[m], p_ref[m + 1]], 1) for m in (t, t + 2)], 0)
            value = jnp.concatenate([rows[x : x + deep] for x in (t * deep // 2, t * deep // 2 + deep)], 1)
            term = jnp.dot(weight, value, preferred_element_type=jnp.float32)
            total = term if total is None else total + term
        return total[:heads, :head] + total[heads:, head:]

    def note(b, high, total):
        where, i = lax.div(b, half), lax.rem(b, half)
        table = stat[where, me]
        for x in range(2):
            rows = slice(8 * x, 8 * x + 8)
            table = jnp.where(lane == 2 * i + x, high[rows], table)
            table = jnp.where(lane == 64 + 2 * i + x, total[rows], table)
        stat[where, me] = table

    def send(buf, g, s, recv):
        for r in range(1, n):
            pltpu.make_async_remote_copy(
                src_ref=buf.at[g, me],
                dst_ref=buf.at[g, me],
                send_sem=send_sem.at[s],
                recv_sem=recv.at[g],
                device_id={"sp": lax.rem(me + r, n)},
                device_id_type=pl.DeviceIdType.MESH,
            ).start()

    def arrived(buf, g, recv):
        pltpu.make_async_copy(buf.at[g, : n - 1], buf.at[g, : n - 1], recv.at[g]).wait()

    def shares(where):
        tables = [stat[where, d] for d in range(n)]
        high = functools.reduce(jnp.maximum, tables)
        counts = [jnp.exp2(t - high) for t in tables]
        total = functools.reduce(jnp.add, [pltpu.roll(t, 64, 1) * c for t, c in zip(tables, counts)])
        return [c / total for c in counts]

    def together(parts, share, b):
        out = []
        for x in range(2):
            column = 2 * (b % half) + x
            terms = [parts[d].astype(jnp.float32)[8 * x : 8 * x + 8] * share[d][:, column : column + 1] for d in range(n)]
            out.append(functools.reduce(jnp.add, terms))
        o_ref[b] = jnp.concatenate(out, 0).astype(jnp.bfloat16)

    fetch_q = pltpu.make_async_copy(q_hbm, q_ref, q_sem)
    k_copy(0).start()
    fetch_q.start()
    for b in range(1, LAG + PAIR):
        k_copy(b).start()
    for b in range(PAIR):
        v_copy(b).start()
    barrier = pltpu.get_barrier_semaphore()
    for r in range(1, n):
        pl.semaphore_signal(barrier, inc=1, device_id={"sp": lax.rem(me + r, n)}, device_id_type=pl.DeviceIdType.MESH)
    for where in range(2):
        stat[where, me] = jnp.zeros((8, 128), jnp.float32)
    fetch_q.wait()

    for b in range(0, LAG, PAIR):
        for u in range(PAIR):
            k_copy(b + u).wait()
        for u in range(PAIR):
            high = scores(b + u, s_buf.at[u])
            note(b + u, high, weights(high, s_buf.at[u], p_buf.at[b + u]))
        for u in range(PAIR):
            k_copy(b + SLOTS + u).start()
        for u in range(PAIR):
            v_copy(b + PAIR + u).start()
    pl.semaphore_wait(barrier, n - 1)

    def pair(it, _):
        b = it * PAIR
        for u in range(PAIR):
            k_copy(b + LAG + u).wait()
            v_copy(b + u).wait()
        for u in range(PAIR):
            p_ref = p_buf.at[lax.rem(it, LAG // PAIR) * PAIR + u]
            high = scores(b + LAG + u, s_buf.at[u])
            part[it, me, u * heads : (u + 1) * heads] = values(b + u, p_ref).astype(jnp.bfloat16)
            note(b + LAG + u, high, weights(high, s_buf.at[u], p_ref))

        @pl.when(b + LAG + SLOTS < batch)
        def _():
            for u in range(PAIR):
                k_copy(b + LAG + SLOTS + u).start()

        @pl.when(b + SLOTS < batch)
        def _():
            for u in range(PAIR):
                v_copy(b + SLOTS + u).start()

        send(part, it, 0, part_sem)

        @pl.when(b + LAG + PAIR == half)
        def _():
            send(stat, 0, 2, stat_sem)

        return 0

    loops = (batch - LAG) // PAIR
    lax.fori_loop(0, loops, pair, 0)
    send(stat, 1, 2, stat_sem)
    for it in range(loops, pairs):
        b = it * PAIR
        for u in range(PAIR):
            v_copy(b + u).wait()
        for u in range(PAIR):
            part[it, me, u * heads : (u + 1) * heads] = values(b + u, p_buf.at[(b + u) % LAG]).astype(jnp.bfloat16)
        send(part, it, 0, part_sem)
    for u in range(PAIR):
        b = pairs * PAIR + u
        v_copy(b).wait()
        last[u, me] = values(b, p_buf.at[b % LAG]).astype(jnp.bfloat16)
        send(last, u, 1, last_sem)

    for where in range(2):
        arrived(stat, where, stat_sem)
        share = shares(where)
        first, end = where * half // PAIR, min((where + 1) * half // PAIR, pairs)
        for it in range(first, end):
            arrived(part, it, part_sem)
        for it in range(first, end):
            for u in range(PAIR):
                together([part[it, d, u * heads : (u + 1) * heads] for d in range(n)], share, it * PAIR + u)
    for u in range(PAIR):
        arrived(last, u, last_sem)
        together([last[u, d] for d in range(n)], share, pairs * PAIR + u)
    for s, buf in enumerate((part, last, stat)):
        pltpu.make_async_copy(buf.at[:, : n - 1], buf.at[:, : n - 1], send_sem.at[s]).wait()


def solution(mesh):
    n = mesh.shape["sp"]

    def step(q, k, v):
        batch, tokens, heads, head = k.shape
        pairs = batch // PAIR - 1
        anywhere = pl.BlockSpec(memory_space=pl.ANY)
        return pl.pallas_call(
            functools.partial(attend, n),
            out_shape=pltpu.VMEM(q.shape, q.dtype),
            in_specs=[anywhere] * 3,
            out_specs=pl.BlockSpec(memory_space=pltpu.VMEM),
            scratch_shapes=[
                pltpu.VMEM(q.shape, q.dtype),
                pltpu.VMEM((SLOTS, tokens, heads, head), jnp.bfloat16),
                pltpu.VMEM((SLOTS, tokens, heads, head), jnp.bfloat16),
                pltpu.VMEM((PAIR, tokens // TILE, heads, TILE * heads), jnp.float32),
                pltpu.VMEM((LAG, tokens // TILE, heads, TILE * heads), jnp.bfloat16),
                pltpu.VMEM((pairs, n, PAIR * heads, head), jnp.bfloat16),
                pltpu.VMEM((PAIR, n, heads, head), jnp.bfloat16),
                pltpu.VMEM((2, n, 8, 128), jnp.float32),
                pltpu.SemaphoreType.DMA(()),
                pltpu.SemaphoreType.DMA((SLOTS,)),
                pltpu.SemaphoreType.DMA((SLOTS,)),
                pltpu.SemaphoreType.DMA((3,)),
                pltpu.SemaphoreType.DMA((pairs,)),
                pltpu.SemaphoreType.DMA((PAIR,)),
                pltpu.SemaphoreType.DMA((2,)),
            ],
            compiler_params=pltpu.CompilerParams(
                vmem_limit_bytes=56 << 20, collective_id=0, has_side_effects=True
            ),
            name="attend",
        )(q, k, v)

    return jax.shard_map(
        step,
        mesh=mesh,
        in_specs=(P("dp", None, None), P("dp", "sp", None, None), P("dp", "sp", None, None)),
        out_specs=P("dp", None, None),
        check_vma=False,
    )
```

```python
import functools
import math

import jax
import jax.numpy as jnp
from jax import lax
from jax.experimental import pallas as pl
from jax.experimental.pallas import tpu as pltpu
from jax.sharding import PartitionSpec as P

TILE = 8
STEP = 32
PAIR = 2
LAG = 6
SLOTS = 8
BEHIND = 4


def attend(n, q_hbm, k_hbm, v_hbm, o_ref, q_ref, k_buf, v_buf, s_buf, p_buf, part, last, stat, q_sem, k_sem, v_sem,
           send_sem, part_sem, last_sem, stat_sem):
    batch, tokens, heads, head = k_hbm.shape
    runs = tokens // TILE
    pairs = batch // PAIR - 1
    half = batch // 2
    chips = n // 2
    chip, core = lax.div(lax.axis_index("sp"), 2), lax.rem(lax.axis_index("sp"), 2)
    me = core * chips + chip
    other = {"sp": 2 * chip + 1 - core}
    scale = head**-0.5 / math.log(2)
    lanes = lax.broadcasted_iota(jnp.int32, (heads, TILE * heads), 1)
    mine = lanes % heads == lax.broadcasted_iota(jnp.int32, (heads, TILE * heads), 0)
    lane = lax.broadcasted_iota(jnp.int32, (8, 128), 1)

    def k_copy(b):
        slot = lax.rem(b, SLOTS)
        return pltpu.make_async_copy(k_hbm.at[b], k_buf.at[slot], k_sem.at[slot])

    def v_copies(b):
        slot, part_of = lax.rem(b, SLOTS), tokens // 2
        return [
            pltpu.make_async_copy(
                v_hbm.at[b, x * part_of : (x + 1) * part_of],
                v_buf.at[slot, x * part_of : (x + 1) * part_of],
                v_sem.at[slot, x],
            )
            for x in range(2)
        ]

    def fetch_v(b):
        for copy in v_copies(b):
            copy.start()

    def fetched_v(b):
        for copy in v_copies(b):
            copy.wait()

    def scores(b, s_ref):
        keys = k_buf.at[lax.rem(b, SLOTS)].reshape(runs, TILE, heads, head)
        query = q_ref[b]
        none = jnp.zeros_like(query)
        high = jnp.full((heads, TILE * heads), -jnp.inf, jnp.float32)
        for m in range(0, runs, STEP):
            total = None
            for j in range(0, TILE, 2):
                two = jnp.concatenate([keys[m : m + STEP, j + c].reshape(STEP * heads, head) for c in range(2)], 1)
                spread = jnp.concatenate(
                    [jnp.concatenate([query if r == j + c else none for c in range(2)], 1) for r in range(TILE)], 0
                )
                term = lax.dot_general(two, spread, (((1,), (1,)), ((), ())), preferred_element_type=jnp.float32)
                total = term if total is None else total + term
            total = jnp.where(mine[None], total.reshape(STEP, heads, TILE * heads), -jnp.inf)
            s_ref[m : m + STEP] = total
            high = jnp.maximum(high, jnp.max(total, 0))
        return jnp.max(high, 1, keepdims=True) * scale

    def weights(high, s_ref, p_ref):
        total = jnp.zeros((heads, TILE * heads), jnp.float32)
        high = jnp.broadcast_to(high, total.shape)
        for m in range(runs):
            weight = jnp.exp2(s_ref[m] * scale - high)
            total = total + weight
            p_ref[m] = weight.astype(jnp.bfloat16)
        return jnp.sum(total, 1, keepdims=True)

    def values(b, p_ref, arrivals=()):
        rows = v_buf.at[lax.rem(b, SLOTS)].reshape(tokens * heads, head)
        deep = 2 * TILE * heads
        total = None
        for t in range(0, runs, 4):
            if arrivals and t % (runs // len(arrivals)) == 0:
                arrivals[t * len(arrivals) // runs].wait()
            weight = jnp.concatenate([jnp.concatenate([p_ref[m], p_ref[m + 1]], 1) for m in (t, t + 2)], 0)
            value = jnp.concatenate([rows[x : x + deep] for x in (t * deep // 2, t * deep // 2 + deep)], 1)
            term = jnp.dot(weight, value, preferred_element_type=jnp.float32)
            total = term if total is None else total + term
        return total[:heads, :head] + total[heads:, head:]

    def note(b, high, total):
        where, i = lax.div(b, half), lax.rem(b, half)
        table = stat[where, me]
        for x in range(2):
            rows = slice(8 * x, 8 * x + 8)
            table = jnp.where(lane == 2 * i + x, high[rows], table)
            table = jnp.where(lane == 64 + 2 * i + x, total[rows], table)
        stat[where, me] = table

    def remote(ref, to, s, recv):
        pltpu.make_async_remote_copy(
            src_ref=ref, dst_ref=ref, send_sem=send_sem.at[s], recv_sem=recv, device_id=to,
            device_id_type=pl.DeviceIdType.MESH,
        ).start()

    def send(buf, g, s, recv):
        for r in range(1, chips):
            remote(buf.at[g, me], {"sp": 2 * lax.rem(chip + r, chips) + core}, s, recv.at[0, g])

    def hand_on(buf, g, s, recv):
        pltpu.make_async_copy(buf.at[g, : chips - 1], buf.at[g, : chips - 1], recv.at[0, g]).wait()
        remote(buf.at[g, pl.ds(core * chips, chips)], other, s, recv.at[1, g])

    def arrived(buf, g, recv):
        pltpu.make_async_copy(buf.at[g, :chips], buf.at[g, :chips], recv.at[1, g]).wait()

    def send_all(u):
        for r in range(1, chips):
            for c in (core, 1 - core):
                remote(last.at[u, me], {"sp": 2 * lax.rem(chip + r, chips) + c}, 2, last_sem.at[u])
        remote(last.at[u, me], other, 2, last_sem.at[u])

    def shares(where):
        tables = [stat[where, d] for d in range(n)]
        high = functools.reduce(jnp.maximum, tables)
        counts = [jnp.exp2(t - high) for t in tables]
        total = functools.reduce(jnp.add, [pltpu.roll(t, 64, 1) * c for t, c in zip(tables, counts)])
        return [c / total for c in counts]

    def together(parts, share, b):
        out = []
        for x in range(2):
            column = 2 * (b % half) + x
            terms = [parts[d].astype(jnp.float32)[8 * x : 8 * x + 8] * share[d][:, column : column + 1] for d in range(n)]
            out.append(functools.reduce(jnp.add, terms))
        o_ref[b] = jnp.concatenate(out, 0).astype(jnp.bfloat16)

    fetch_q = pltpu.make_async_copy(q_hbm, q_ref, q_sem)
    k_copy(0).start()
    fetch_q.start()
    for b in range(1, LAG + PAIR):
        k_copy(b).start()
    for b in range(PAIR):
        fetch_v(b)
    barrier = pltpu.get_barrier_semaphore()
    for r in range(1, n):
        peer = {"sp": lax.rem(lax.axis_index("sp") + r, n)}
        pl.semaphore_signal(barrier, inc=1, device_id=peer, device_id_type=pl.DeviceIdType.MESH)
    for where in range(2):
        stat[where, me] = jnp.zeros((8, 128), jnp.float32)
    fetch_q.wait()

    for b in range(0, LAG, PAIR):
        for u in range(PAIR):
            k_copy(b + u).wait()
        for u in range(PAIR):
            high = scores(b + u, s_buf.at[u])
            note(b + u, high, weights(high, s_buf.at[u], p_buf.at[b + u]))
        for u in range(PAIR):
            k_copy(b + SLOTS + u).start()
        for u in range(PAIR):
            fetch_v(b + PAIR + u)
    pl.semaphore_wait(barrier, n - 1)

    def pair(it, _):
        b = it * PAIR
        for u in range(PAIR):
            k_copy(b + LAG + u).wait()
            fetched_v(b + u)
        for u in range(PAIR):
            p_ref = p_buf.at[lax.rem(it, LAG // PAIR) * PAIR + u]
            high = scores(b + LAG + u, s_buf.at[u])
            part[it, me, u * heads : (u + 1) * heads] = values(b + u, p_ref).astype(jnp.bfloat16)
            note(b + LAG + u, high, weights(high, s_buf.at[u], p_ref))

        @pl.when(b + LAG + SLOTS < batch)
        def _():
            for u in range(PAIR):
                k_copy(b + LAG + SLOTS + u).start()

        @pl.when(b + SLOTS < batch)
        def _():
            for u in range(PAIR):
                fetch_v(b + SLOTS + u)

        send(part, it, 0, part_sem)

        @pl.when(b + LAG + PAIR == half)
        def _():
            send(stat, 0, 1, stat_sem)

        @pl.when(it >= BEHIND)
        def _():
            hand_on(part, it - BEHIND, 0, part_sem)

        return 0

    loops = (batch - LAG) // PAIR
    lax.fori_loop(0, loops, pair, 0)
    send(stat, 1, 1, stat_sem)
    for it in range(loops, pairs):
        b = it * PAIR
        for u in range(PAIR):
            fetched_v(b + u)
        for u in range(PAIR):
            part[it, me, u * heads : (u + 1) * heads] = values(b + u, p_buf.at[(b + u) % LAG]).astype(jnp.bfloat16)
        send(part, it, 0, part_sem)
    for u in range(PAIR):
        b = pairs * PAIR + u
        last[u, me] = values(b, p_buf.at[b % LAG], v_copies(b)).astype(jnp.bfloat16)
        send_all(u)

    hand_on(stat, 0, 1, stat_sem)
    for it in range(loops - BEHIND, pairs - 2):
        hand_on(part, it, 0, part_sem)
    hand_on(stat, 1, 1, stat_sem)
    for it in range(pairs - 2, pairs):
        hand_on(part, it, 0, part_sem)
    for where in range(2):
        arrived(stat, where, stat_sem)
        share = shares(where)
        first, end = where * half // PAIR, min((where + 1) * half // PAIR, pairs)
        for it in range(first, end):
            arrived(part, it, part_sem)
        for it in range(first, end):
            for u in range(PAIR):
                together([part[it, d, u * heads : (u + 1) * heads] for d in range(n)], share, it * PAIR + u)
    for u in range(PAIR):
        pltpu.make_async_copy(last.at[u, : n - 1], last.at[u, : n - 1], last_sem.at[u]).wait()
        together([last[u, d] for d in range(n)], share, pairs * PAIR + u)
    for s, buf, sent in ((0, part, n - 1), (1, stat, n - 1), (2, last, n - 1)):
        pltpu.make_async_copy(buf.at[:, :sent], buf.at[:, :sent], send_sem.at[s]).wait()


def solution(mesh):
    n = mesh.shape["sp"]

    def step(q, k, v):
        batch, tokens, heads, head = k.shape
        pairs = batch // PAIR - 1
        anywhere = pl.BlockSpec(memory_space=pl.ANY)
        return pl.pallas_call(
            functools.partial(attend, n),
            out_shape=pltpu.VMEM(q.shape, q.dtype),
            in_specs=[anywhere] * 3,
            out_specs=pl.BlockSpec(memory_space=pltpu.VMEM),
            scratch_shapes=[
                pltpu.VMEM(q.shape, q.dtype),
                pltpu.VMEM((SLOTS, tokens, heads, head), jnp.bfloat16),
                pltpu.VMEM((SLOTS, tokens, heads, head), jnp.bfloat16),
                pltpu.VMEM((PAIR, tokens // TILE, heads, TILE * heads), jnp.float32),
                pltpu.VMEM((LAG, tokens // TILE, heads, TILE * heads), jnp.bfloat16),
                pltpu.VMEM((pairs, n, PAIR * heads, head), jnp.bfloat16),
                pltpu.VMEM((PAIR, n, heads, head), jnp.bfloat16),
                pltpu.VMEM((2, n, 8, 128), jnp.float32),
                pltpu.SemaphoreType.DMA(()),
                pltpu.SemaphoreType.DMA((SLOTS,)),
                pltpu.SemaphoreType.DMA((SLOTS, 2)),
                pltpu.SemaphoreType.DMA((3,)),
                pltpu.SemaphoreType.DMA((2, pairs)),
                pltpu.SemaphoreType.DMA((PAIR,)),
                pltpu.SemaphoreType.DMA((2, 2)),
            ],
            compiler_params=pltpu.CompilerParams(
                vmem_limit_bytes=56 << 20, collective_id=0, has_side_effects=True
            ),
            name="attend",
        )(q, k, v)

    return jax.shard_map(
        step,
        mesh=mesh,
        in_specs=(P("dp", None, None), P("dp", "sp", None, None), P("dp", "sp", None, None)),
        out_specs=P("dp", None, None),
        check_vma=False,
    )
```

```python
import functools
import math

import jax
import jax.numpy as jnp
from jax import lax
from jax.experimental import pallas as pl
from jax.experimental.pallas import tpu as pltpu
from jax.sharding import PartitionSpec as P

TILE = 8
STEP = 32
PAIR = 2
LAG = 6
K_SLOTS = 8
V_SLOTS = 8
CUT = 1
BEHIND = 4


def attend(n, q_hbm, k_hbm, v_hbm, o_ref, q_ref, k_buf, v_buf, s_buf, p_buf, part, last, stat, q_sem, k_sem, v_sem,
           send_sem, part_sem, last_sem, stat_sem):
    batch, tokens, heads, head = k_hbm.shape
    runs = tokens // TILE
    pairs = batch // PAIR - 1
    half = batch // 2
    chips = n // 2
    chip, core = lax.div(lax.axis_index("sp"), 2), lax.rem(lax.axis_index("sp"), 2)
    me = core * chips + chip
    other = {"sp": 2 * chip + 1 - core}
    scale = head**-0.5 / math.log(2)
    lanes = lax.broadcasted_iota(jnp.int32, (heads, TILE * heads), 1)
    mine = lanes % heads == lax.broadcasted_iota(jnp.int32, (heads, TILE * heads), 0)
    lane = lax.broadcasted_iota(jnp.int32, (8, 128), 1)

    def k_copy(b):
        slot = lax.rem(b, K_SLOTS)
        return pltpu.make_async_copy(k_hbm.at[b], k_buf.at[slot], k_sem.at[slot])

    def v_copies(b):
        slot, part_of = lax.rem(b, V_SLOTS), tokens // CUT
        return [
            pltpu.make_async_copy(
                v_hbm.at[b, x * part_of : (x + 1) * part_of],
                v_buf.at[slot, x * part_of : (x + 1) * part_of],
                v_sem.at[slot, x],
            )
            for x in range(CUT)
        ]

    def fetch_v(b):
        for copy in v_copies(b):
            copy.start()

    def fetched_v(b):
        for copy in v_copies(b):
            copy.wait()

    def scores(b, s_ref):
        keys = k_buf.at[lax.rem(b, K_SLOTS)].reshape(runs, TILE, heads, head)
        query = q_ref[b]
        none = jnp.zeros_like(query)
        high = jnp.full((heads, TILE * heads), -jnp.inf, jnp.float32)
        for m in range(0, runs, STEP):
            total = None
            for j in range(0, TILE, 2):
                two = jnp.concatenate([keys[m : m + STEP, j + c].reshape(STEP * heads, head) for c in range(2)], 1)
                spread = jnp.concatenate(
                    [jnp.concatenate([query if r == j + c else none for c in range(2)], 1) for r in range(TILE)], 0
                )
                term = lax.dot_general(two, spread, (((1,), (1,)), ((), ())), preferred_element_type=jnp.float32)
                total = term if total is None else total + term
            total = jnp.where(mine[None], total.reshape(STEP, heads, TILE * heads), -jnp.inf)
            s_ref[m : m + STEP] = total
            high = jnp.maximum(high, jnp.max(total, 0))
        return jnp.max(high, 1, keepdims=True) * scale

    def weights(high, s_ref, p_ref):
        total = jnp.zeros((heads, TILE * heads), jnp.float32)
        high = jnp.broadcast_to(high, total.shape)
        for m in range(runs):
            weight = jnp.exp2(s_ref[m] * scale - high)
            total = total + weight
            p_ref[m] = weight.astype(jnp.bfloat16)
        return jnp.sum(total, 1, keepdims=True)

    def values(b, p_ref, arrivals=()):
        rows = v_buf.at[lax.rem(b, V_SLOTS)].reshape(tokens * heads, head)
        deep = 2 * TILE * heads
        total = None
        for t in range(0, runs, 4):
            if arrivals and t % (runs // len(arrivals)) == 0:
                arrivals[t * len(arrivals) // runs].wait()
            weight = jnp.concatenate([jnp.concatenate([p_ref[m], p_ref[m + 1]], 1) for m in (t, t + 2)], 0)
            value = jnp.concatenate([rows[x : x + deep] for x in (t * deep // 2, t * deep // 2 + deep)], 1)
            term = jnp.dot(weight, value, preferred_element_type=jnp.float32)
            total = term if total is None else total + term
        return total[:heads, :head] + total[heads:, head:]

    def note(b, high, total):
        where, i = lax.div(b, half), lax.rem(b, half)
        table = stat[where, me]
        for x in range(2):
            rows = slice(8 * x, 8 * x + 8)
            table = jnp.where(lane == 2 * i + x, high[rows], table)
            table = jnp.where(lane == 64 + 2 * i + x, total[rows], table)
        stat[where, me] = table

    def remote(ref, to, s, recv):
        pltpu.make_async_remote_copy(
            src_ref=ref, dst_ref=ref, send_sem=send_sem.at[s], recv_sem=recv, device_id=to,
            device_id_type=pl.DeviceIdType.MESH,
        ).start()

    def send(buf, g, s, recv):
        for r in range(1, chips):
            remote(buf.at[g, me], {"sp": 2 * lax.rem(chip + r, chips) + core}, s, recv.at[0, g])

    def hand_on(buf, g, s, recv):
        pltpu.make_async_copy(buf.at[g, : chips - 1], buf.at[g, : chips - 1], recv.at[0, g]).wait()
        remote(buf.at[g, pl.ds(core * chips, chips)], other, s, recv.at[1, g])

    def arrived(buf, g, recv):
        pltpu.make_async_copy(buf.at[g, :chips], buf.at[g, :chips], recv.at[1, g]).wait()

    def send_all(u):
        for r in range(1, chips):
            for c in (core, 1 - core):
                remote(last.at[u, me], {"sp": 2 * lax.rem(chip + r, chips) + c}, 2, last_sem.at[u])
        remote(last.at[u, me], other, 2, last_sem.at[u])

    def shares(where):
        tables = [stat[where, d] for d in range(n)]
        high = functools.reduce(jnp.maximum, tables)
        counts = [jnp.exp2(t - high) for t in tables]
        total = functools.reduce(jnp.add, [pltpu.roll(t, 64, 1) * c for t, c in zip(tables, counts)])
        return [c / total for c in counts]

    def together(parts, share, b):
        out = []
        for x in range(2):
            column = 2 * (b % half) + x
            terms = [parts[d].astype(jnp.float32)[8 * x : 8 * x + 8] * share[d][:, column : column + 1] for d in range(n)]
            out.append(functools.reduce(jnp.add, terms))
        o_ref[b] = jnp.concatenate(out, 0).astype(jnp.bfloat16)

    fetch_q = pltpu.make_async_copy(q_hbm, q_ref, q_sem)
    k_copy(0).start()
    fetch_q.start()
    for b in range(1, K_SLOTS):
        k_copy(b).start()
    for b in range(V_SLOTS - LAG):
        fetch_v(b)
    barrier = pltpu.get_barrier_semaphore()
    for r in range(1, n):
        peer = {"sp": lax.rem(lax.axis_index("sp") + r, n)}
        pl.semaphore_signal(barrier, inc=1, device_id=peer, device_id_type=pl.DeviceIdType.MESH)
    for where in range(2):
        stat[where, me] = jnp.zeros((8, 128), jnp.float32)
    fetch_q.wait()

    for b in range(0, LAG, PAIR):
        for u in range(PAIR):
            k_copy(b + u).wait()
        for u in range(PAIR):
            high = scores(b + u, s_buf.at[u])
            note(b + u, high, weights(high, s_buf.at[u], p_buf.at[b + u]))
        for u in range(PAIR):
            k_copy(b + K_SLOTS + u).start()
        for u in range(PAIR):
            if b + V_SLOTS >= LAG:
                fetch_v(b + V_SLOTS - LAG + u)
    pl.semaphore_wait(barrier, n - 1)

    def pair(it, _):
        b = it * PAIR
        for u in range(PAIR):
            k_copy(b + LAG + u).wait()
            fetched_v(b + u)
        for u in range(PAIR):
            p_ref = p_buf.at[lax.rem(it, LAG // PAIR) * PAIR + u]
            high = scores(b + LAG + u, s_buf.at[u])
            part[it, me, u * heads : (u + 1) * heads] = values(b + u, p_ref).astype(jnp.bfloat16)
            note(b + LAG + u, high, weights(high, s_buf.at[u], p_ref))

        @pl.when(b + LAG + K_SLOTS < batch)
        def _():
            for u in range(PAIR):
                k_copy(b + LAG + K_SLOTS + u).start()

        @pl.when(b + V_SLOTS < batch)
        def _():
            for u in range(PAIR):
                fetch_v(b + V_SLOTS + u)

        send(part, it, 0, part_sem)

        @pl.when(b + LAG + PAIR == half)
        def _():
            send(stat, 0, 1, stat_sem)

        @pl.when(it >= BEHIND)
        def _():
            hand_on(part, it - BEHIND, 0, part_sem)

        return 0

    loops = (batch - LAG) // PAIR
    lax.fori_loop(0, loops, pair, 0)
    send(stat, 1, 1, stat_sem)
    for it in range(loops, pairs):
        b = it * PAIR
        for u in range(PAIR):
            fetched_v(b + u)
        for u in range(PAIR):
            part[it, me, u * heads : (u + 1) * heads] = values(b + u, p_buf.at[(b + u) % LAG]).astype(jnp.bfloat16)
        send(part, it, 0, part_sem)
    for u in range(PAIR):
        b = pairs * PAIR + u
        last[u, me] = values(b, p_buf.at[b % LAG], v_copies(b)).astype(jnp.bfloat16)
        send_all(u)

    def combine(share, first, end):
        for it in range(first, end):
            arrived(part, it, part_sem)
        for it in range(first, end):
            for u in range(PAIR):
                together([part[it, d, u * heads : (u + 1) * heads] for d in range(n)], share, it * PAIR + u)

    middle, late = half // PAIR, pairs - 2
    hand_on(stat, 0, 1, stat_sem)
    arrived(stat, 0, stat_sem)
    combine(shares(0), 0, middle)
    for it in range(loops - BEHIND, late):
        hand_on(part, it, 0, part_sem)
    hand_on(stat, 1, 1, stat_sem)
    for it in range(late, pairs):
        hand_on(part, it, 0, part_sem)
    arrived(stat, 1, stat_sem)
    share = shares(1)
    combine(share, middle, late)
    combine(share, late, pairs)
    for u in range(PAIR):
        pltpu.make_async_copy(last.at[u, : n - 1], last.at[u, : n - 1], last_sem.at[u]).wait()
        together([last[u, d] for d in range(n)], share, pairs * PAIR + u)
    for s, buf, sent in ((0, part, n - 1), (1, stat, n - 1), (2, last, n - 1)):
        pltpu.make_async_copy(buf.at[:, :sent], buf.at[:, :sent], send_sem.at[s]).wait()


def solution(mesh):
    n = mesh.shape["sp"]

    def step(q, k, v):
        batch, tokens, heads, head = k.shape
        pairs = batch // PAIR - 1
        anywhere = pl.BlockSpec(memory_space=pl.ANY)
        return pl.pallas_call(
            functools.partial(attend, n),
            out_shape=pltpu.VMEM(q.shape, q.dtype),
            in_specs=[anywhere] * 3,
            out_specs=pl.BlockSpec(memory_space=pltpu.VMEM),
            scratch_shapes=[
                pltpu.VMEM(q.shape, q.dtype),
                pltpu.VMEM((K_SLOTS, tokens, heads, head), jnp.bfloat16),
                pltpu.VMEM((V_SLOTS, tokens, heads, head), jnp.bfloat16),
                pltpu.VMEM((PAIR, tokens // TILE, heads, TILE * heads), jnp.float32),
                pltpu.VMEM((LAG, tokens // TILE, heads, TILE * heads), jnp.bfloat16),
                pltpu.VMEM((pairs, n, PAIR * heads, head), jnp.bfloat16),
                pltpu.VMEM((PAIR, n, heads, head), jnp.bfloat16),
                pltpu.VMEM((2, n, 8, 128), jnp.float32),
                pltpu.SemaphoreType.DMA(()),
                pltpu.SemaphoreType.DMA((K_SLOTS,)),
                pltpu.SemaphoreType.DMA((V_SLOTS, CUT)),
                pltpu.SemaphoreType.DMA((3,)),
                pltpu.SemaphoreType.DMA((2, pairs)),
                pltpu.SemaphoreType.DMA((PAIR,)),
                pltpu.SemaphoreType.DMA((2, 2)),
            ],
            compiler_params=pltpu.CompilerParams(
                vmem_limit_bytes=56 << 20, collective_id=0, has_side_effects=True
            ),
            name="attend",
        )(q, k, v)

    return jax.shard_map(
        step,
        mesh=mesh,
        in_specs=(P("dp", None, None), P("dp", "sp", None, None), P("dp", "sp", None, None)),
        out_specs=P("dp", None, None),
        check_vma=False,
    )
```
